256 devices in a mesh: tm: 16 (over z, y_hi), rows: 16 (over y_lo, x, core).
Axes of the slice: x: 4, y: 4 (y_hi: 2, y_lo: 2; y = y_hi * 2 + y_lo), z: 8, core: 2. Of those that a mesh axis runs over, the one named last changes fastest.
Arguments:
- upstream: bfloat16 [64, 128, 128, 128], P('tm', 'rows'), may hold values from -6 to 6
- saved_first: bfloat16 [64, 128, 128, 128], P('tm', 'rows'), may hold values from -8 to 8
- saved_second: bfloat16 [64, 128, 128, 128], P('tm', 'rows'), may hold values from -8 to 8
- weight_first: bfloat16 [3456, 128], replicated, may hold values from -0.109375 to 0.109375
- weight_second: bfloat16 [3456, 128], replicated, may hold values from -0.109375 to 0.109375
Outputs:
- grad_input: bfloat16 [64, 128, 128, 128], P('tm', 'rows')
- wgrad_first: float32 [3456, 128], P('tm')
- wgrad_second: float32 [3456, 128], P('tm')
The draws below stay inside these ranges and needn't reach their ends.
All inputs are finite; a program needn't handle non-finite values.
Results may differ from the reference program's by a relative error of at most 0.005.
Values may be sent and summed in bfloat16 or wider, within the bound.
No kernel may reach another device: no remote copies, remote signals or barrier semaphores. Data moves between devices by JAX's collectives and lax.ppermute only.
A program may use at most 64 MiB of HBM per device.

```python
import math
import jax
import jax.numpy as jnp
from jax import lax

CH = 128
COLS = 128
NF = 64
NR = 128


def draw_upstream(key, part):
    shape = (NF, NR, COLS, CH)
    offset = 4.0 / math.sqrt(NF * NR * COLS)
    values = jnp.clip(jax.random.normal(key, shape, jnp.float32), -5.9, 5.9)
    return jnp.clip(values + offset, -6.0, 6.0).astype(jnp.bfloat16)


def level_of(stream_key, extent, split, least, top_value):
    factor_of, own = 1.0, jax.random.fold_in(stream_key, 6)
    for position, parts in split:
        draws = jnp.exp(jax.random.uniform(jax.random.fold_in(own, position), (parts,), jnp.float32, least / len(split), top_value / len(split)))
        factor_of = factor_of * jnp.repeat(draws, extent[position] // parts).reshape([-1 if axis == position else 1 for axis in range(len(extent))])
    return factor_of


def centred(rng, shape, deviation, most, cuts=(), kind=jnp.bfloat16):
    array = deviation * jax.random.normal(rng, shape, jnp.float32)
    if cuts:
        array = array * level_of(rng, shape, cuts, -0.22, 0.18)
    return jnp.clip(array, -most, most).astype(kind)


def setup_inputs(seed: int = 0) -> dict:
    seeds = jax.random.split(jax.random.key(seed), 6)
    return {
        "upstream": draw_upstream(jax.random.fold_in(seeds[5], 71), 0),
        "saved_first": centred(seeds[1], (NF, NR, COLS, CH), 1.5, 8.0, ((0, 16), (1, 16))),
        "saved_second": centred(seeds[2], (NF, NR, COLS, CH), 1.5, 8.0, ((0, 16), (1, 16))),
        "weight_first": centred(seeds[3], (27 * CH, CH), (27 * CH) ** -0.5, 0.109375),
        "weight_second": centred(seeds[4], (27 * CH, CH), (27 * CH) ** -0.5, 0.109375),
    }


def silu_slope(value):
    sigma = jax.nn.sigmoid(value)
    return sigma * (1.0 + value * (1.0 - sigma))

def taps_frame(padded, frame, height, width):
    slab = lax.dynamic_slice_in_dim(padded, frame, 3, 0)
    pieces = []
    for shift_t in range(3):
        for shift_r in range(3):
            for shift_c in range(3):
                pieces.append(slab[2 - shift_t, 2 - shift_r:2 - shift_r + height, 2 - shift_c:2 - shift_c + width])
    return jnp.concatenate(pieces, axis=-1).reshape(height * width, -1)

def layer_back(grad_out, saved, weight):
    frames, height, width, chans = grad_out.shape
    padded = jnp.pad(grad_out, ((0, 2), (1, 1), (1, 1), (0, 0)))
    flipped = weight.reshape(27, chans, chans).transpose(0, 2, 1).reshape(27 * chans, chans)
    active = jax.nn.silu(saved.astype(jnp.float32)).astype(jnp.bfloat16)

    def one_frame(total, frame):
        columns = taps_frame(padded, frame, height, width)
        spread = jnp.dot(columns, flipped, preferred_element_type=jnp.float32)
        local_act = lax.dynamic_index_in_dim(active, frame, 0, keepdims=False).reshape(height * width, chans)
        total = total + jnp.dot(local_act.T, columns, preferred_element_type=jnp.float32)
        local_saved = lax.dynamic_index_in_dim(saved, frame, 0, keepdims=False).astype(jnp.float32)
        result = (spread.reshape(height, width, chans) * silu_slope(local_saved)).astype(jnp.bfloat16)
        return (total, result)
    start = jnp.zeros((chans, 27 * chans), jnp.float32)
    total, grads = lax.scan(one_frame, start, jnp.arange(frames, dtype=jnp.int32))
    wsum = total.reshape(chans, 27, chans).transpose(1, 0, 2).reshape(27 * chans, chans)
    return (grads, wsum)

def reference(upstream, saved_first, saved_second, weight_first, weight_second):
    grad_mid, wsum_second = layer_back(upstream, saved_second, weight_second)
    grad_input, wsum_first = layer_back(grad_mid, saved_first, weight_first)
    factor = 1.0 / math.sqrt(upstream.shape[0] * upstream.shape[1] * upstream.shape[2])
    return (grad_input, wsum_first * factor, wsum_second * factor)
```

```python
import math

import jax
import jax.numpy as jnp
from jax import lax
from jax.experimental import pallas as pl
from jax.experimental.pallas import tpu as pltpu
from jax.sharding import Mesh
from jax.sharding import PartitionSpec as P

TM = ("z", "yh")
CHIPS = ("yl", "x")
ROWS = ("yl", "x", "core")
BF16 = jnp.bfloat16
F32 = jnp.float32
CH = 128


def local_call(kernel, outs, scratch, *args):
    return pl.pallas_call(
        kernel,
        out_shape=outs,
        scratch_shapes=scratch,
        compiler_params=pltpu.CompilerParams(vmem_limit_bytes=60 * 1024 * 1024),
    )(*args)


def store_shifted(dest, base, part):
    size = part.shape[0]
    wide = part.astype(F32)
    column = lax.broadcasted_iota(jnp.int32, (size, CH), 0) % 128
    after = jnp.where(column == 127, 0.0, pltpu.roll(wide, size - 1, 0))
    before = jnp.where(column == 0, 0.0, pltpu.roll(wide, 1, 0))
    dest[base : base + size, 0:CH] = after.astype(BF16)
    dest[base : base + size, CH : 2 * CH] = part
    dest[base : base + size, 2 * CH : 3 * CH] = before.astype(BF16)


def store_frame(dest, frame, above, own, below):
    base = frame * (own.shape[0] + 256)
    store_shifted(dest, base, above)
    for at in range(0, own.shape[0], 256):
        store_shifted(dest, base + 128 + at, own[at : at + 256])
    store_shifted(dest, base + 128 + own.shape[0], below)


def toeplitz_kernel(weight, out):
    for frame in range(4):
        for tap in range(9):
            rows = slice((9 * frame + tap) * CH, (9 * frame + tap + 1) * CH)
            for j in range(2):
                p = j + 2 - frame
                if 0 <= p <= 2:
                    at = (9 * p + tap) * CH
                    out[rows, j * CH : (j + 1) * CH] = weight[at : at + CH, :].T
                else:
                    out[rows, j * CH : (j + 1) * CH] = jnp.zeros((CH, CH), BF16)


def toeplitz(weight):
    return local_call(toeplitz_kernel, jax.ShapeDtypeStruct((36 * CH, 2 * CH), BF16), [], weight)


def spread_kernel(layout, *refs):
    sources, (saved, taps, out, wide) = refs[:-4], refs[-4:]
    for frame, (source, at) in enumerate(layout):
        above, own, below = sources[3 * source : 3 * source + 3]
        store_frame(wide, frame, above[at], own[at], below[at])
    positions = out.shape[1]
    stride = positions + 256
    block = 512
    for at in range(0, positions, block):
        lhs = jnp.concatenate(
            [
                wide[frame * stride + at + (2 - q) * 128 : frame * stride + at + (2 - q) * 128 + block, :]
                for frame in range(4)
                for q in range(3)
            ],
            axis=1,
        )
        spread = jnp.dot(lhs, taps[...], preferred_element_type=F32)
        for j in range(2):
            value = saved[j, at : at + block, :].astype(F32)
            sigma = jax.nn.sigmoid(value)
            slope = sigma * (1.0 + value * (1.0 - sigma))
            out[j, at : at + block, :] = (spread[:, j * CH : (j + 1) * CH] * slope).astype(BF16)


def spread_pair(layout, sources, saved, taps):
    positions = saved.shape[1]
    flat = [array for source in sources for array in source]
    return local_call(
        lambda *refs: spread_kernel(layout, *refs),
        jax.ShapeDtypeStruct(saved.shape, BF16),
        [pltpu.VMEM((4 * (positions + 256), 3 * CH), BF16)],
        *flat,
        saved,
        taps,
    )


def wsum_kernel(layout, first, count, *refs):
    sources, (earlier, saved, out, wide, turned, total) = refs[:-6], refs[-6:]
    positions = saved.shape[1]
    stride = positions + 256
    for s in range(count):
        ref, at = (earlier, s) if first + s < 0 else (saved, first + s)
        value = ref[at].astype(F32)
        turned[s * CH : (s + 1) * CH, :] = (value * jax.nn.sigmoid(value)).astype(BF16).T
    total[...] = jnp.zeros(total.shape, F32)
    for frame, (source, at) in enumerate(layout):
        above, own, below = sources[3 * source : 3 * source + 3]
        store_frame(wide, frame, above[at], own[at], below[at])
    for frame in range(len(layout)):
        lowest = max(0, first - (frame - 2))
        top = min(2, first + count - 1 - (frame - 2))
        s = frame - 2 + lowest - first
        rhs = jnp.concatenate(
            [
                wide[frame * stride + (2 - q) * 128 : frame * stride + (2 - q) * 128 + positions, :]
                for q in range(3)
            ],
            axis=1,
        )
        lhs = turned[s * CH : (s + top - lowest + 1) * CH, :]
        total[lowest * CH : (top + 1) * CH, :] += jnp.dot(lhs, rhs, preferred_element_type=F32)
    for p in range(3):
        for tap in range(9):
            at = (9 * p + tap) * CH
            out[at : at + CH, :] = total[p * CH : (p + 1) * CH, tap * CH : (tap + 1) * CH]


def wsum(layout, sources, earlier, saved, first):
    positions = saved.shape[1]
    flat = [array for source in sources for array in source]
    count = saved.shape[0] - first
    return local_call(
        lambda *refs: wsum_kernel(layout, first, count, *refs),
        jax.ShapeDtypeStruct((27 * CH, CH), F32),
        [
            pltpu.VMEM((len(layout) * (positions + 256), 3 * CH), BF16),
            pltpu.VMEM((count * CH, positions), BF16),
            pltpu.VMEM((3 * CH, 9 * CH), F32),
        ],
        *flat,
        earlier,
        saved,
    )


def moved(block, axis, step):
    count = lax.axis_size(axis)
    route = [(i, i + step) for i in range(count) if 0 <= i + step < count]
    return lax.ppermute(block, axis, route)


def row_halo(field):
    above = moved(field[:, -128:, :], ROWS, 1)
    below = moved(field[:, :128, :], ROWS, -1)
    return above, below


def exchanged(pieces, axis):
    return lax.all_to_all(pieces, axis, split_axis=0, concat_axis=0, tiled=True)


def summed(pieces, axis):
    return exchanged(pieces.astype(BF16), axis).astype(F32).sum(axis=0)


def reduced(first, second):
    blocks, chips = lax.axis_size(TM), lax.axis_size(CHIPS)
    share = first.shape[0] // blocks
    both = jnp.stack([first.reshape(blocks, share, CH), second.reshape(blocks, share, CH)], 1)
    pieces = both.reshape(blocks, 2 * chips, share // chips, CH)
    core = lax.axis_index("core")
    halves = pieces.reshape(blocks, 2, chips, share // chips, CH)
    mine = lax.dynamic_index_in_dim(halves, core, 1, keepdims=False)
    other = lax.dynamic_index_in_dim(halves, 1 - core, 1, keepdims=False)
    half = mine + lax.ppermute(other, "core", [(0, 1), (1, 0)])
    part = summed(half.transpose(1, 0, 2, 3).reshape(chips, -1, CH), CHIPS)
    part = summed(part.reshape(blocks, share // chips, CH), TM)
    every = exchanged(jnp.broadcast_to(part, (2 * chips, *part.shape)), ROWS)
    every = every.reshape(chips, 2, share // chips, CH).transpose(1, 0, 2, 3)
    every = every.reshape(2, share, CH)
    return every[0], every[1]


def body(upstream, saved_first, saved_second, weight_first, weight_second):
    frames, height, width, chans = upstream.shape
    flat = lambda a: a.reshape(frames, height * width, chans)
    up, s1, s2 = flat(upstream), flat(saved_first), flat(saved_second)

    above, below = row_halo(up)
    later = moved(up[:2], TM, -1)
    later_edge = moved(jnp.stack([above[:2], below[:2]]), TM, -1)
    s1_before = moved(s1[-2:], TM, 1)
    taps_second = toeplitz(weight_second)
    taps_first = toeplitz(weight_first)

    here = (above, up, below)
    next_frames = (later_edge[0], later, later_edge[1])
    low = ((0, 0), (0, 1), (0, 2), (0, 3))
    high = ((0, 2), (0, 3), (1, 0), (1, 1))
    mid_low = spread_pair(low, [here], s2[:2], taps_second)
    mid_high = spread_pair(high, [here, next_frames], s2[2:], taps_second)
    wsum_second = wsum(low + high[2:], [here, next_frames], s2[:1], s2, 0)

    mid = jnp.concatenate([mid_low, mid_high])
    above, below = row_halo(mid)
    later = moved(mid_low, TM, -1)
    later_edge = moved(jnp.stack([above[:2], below[:2]]), TM, -1)
    here = (above, mid, below)
    next_frames = (later_edge[0], later, later_edge[1])
    wsum_first = wsum(low, [here], s1_before, s1, -2)
    in_low = spread_pair(low, [here], s1[:2], taps_first)
    in_high = spread_pair(high, [here, next_frames], s1[2:], taps_first)
    grad_input = jnp.concatenate([in_low, in_high]).reshape(upstream.shape)

    factor = 1.0 / math.sqrt(
        frames * lax.axis_size(TM) * height * lax.axis_size(ROWS) * width
    )
    share_first, share_second = reduced(wsum_first, wsum_second)
    return (grad_input, share_first * factor, share_second * factor)


def solution(mesh):
    finer = Mesh(mesh.devices.reshape(8, 2, 2, 4, 2), ("z", "yh", "yl", "x", "core"))
    field = P(TM, ROWS, None, None)
    in_specs = (field, field, field, P(), P())
    out_specs = (field, P(TM, None), P(TM, None))
    return jax.shard_map(body, mesh=finer, in_specs=in_specs, out_specs=out_specs, check_vma=False)
```

```python
import math

import jax
import jax.numpy as jnp
from jax import lax
from jax.experimental import pallas as pl
from jax.experimental.pallas import tpu as pltpu
from jax.sharding import Mesh
from jax.sharding import PartitionSpec as P


TM = ("z", "yh")
PLANE = ("yh", "yl", "x")
ROWS = ("yl", "x", "core")
BF16 = jnp.bfloat16
F32 = jnp.float32
CH = 128


PAD = 32
ROW = 128


def local_call(kernel, outs, scratch, mebibytes, *args):
    scalar = pl.BlockSpec(memory_space=pltpu.SMEM)
    return pl.pallas_call(
        kernel,
        out_shape=outs,
        in_specs=[scalar if a.dtype == jnp.int32 else pl.BlockSpec() for a in args],
        scratch_shapes=scratch,
        compiler_params=pltpu.CompilerParams(vmem_limit_bytes=mebibytes * 1024 * 1024),
    )(*args)


def after(value, *others):
    return lax.optimization_barrier((value, *others))[0]


def store_shifted(dest, base, part):
    size = part.shape[0]
    wide = part.astype(F32)
    column = lax.broadcasted_iota(jnp.int32, (size, CH), 0) % 128
    later = jnp.where(column == 127, 0.0, pltpu.roll(wide, size - 1, 0))
    before = jnp.where(column == 0, 0.0, pltpu.roll(wide, 1, 0))
    dest[base : base + size, 0:CH] = later.astype(BF16)
    dest[base : base + size, CH : 2 * CH] = part
    dest[base : base + size, 2 * CH : 3 * CH] = before.astype(BF16)


def with_rows(above, own, below, frame, at, rows):
    size = rows * ROW
    return [
        (above, frame, 2 * ROW - size, size),
        (own, at, 0, own.shape[1]),
        (below, frame, 0, size),
    ]


def next_frame(edges, own, frame, rows):
    size = rows * ROW
    return [
        (edges, frame, 2 * ROW - size, size),
        (own, frame, 0, own.shape[1]),
        (edges, frame, 2 * ROW, size),
    ]


def whole(ref, frame):
    return [(ref, frame, 0, ref.shape[1])]


def store_frames(dest, frames, first=0):
    stride = sum(piece[3] for piece in frames[0])
    for frame, pieces in enumerate(frames):
        base = (first + frame) * stride
        for ref, at, begin, rows in pieces:
            step = min(rows, 256)
            for start in range(begin, begin + rows, step):
                store_shifted(dest, base, ref[at, start : start + step])
                base += step


def toeplitz_kernel(weight, out):
    zero = jnp.zeros((CH, CH), BF16)
    for tap in range(9):
        for p in range(3):
            at = (9 * p + tap) * CH
            turned = weight[at : at + CH, :].T
            for j in range(2):
                row = (9 * (j + 2 - p) + tap) * CH
                out[row : row + CH, j * CH : (j + 1) * CH] = turned
        out[(27 + tap) * CH : (28 + tap) * CH, 0:CH] = zero
        out[tap * CH : (tap + 1) * CH, CH : 2 * CH] = zero


def toeplitz(weight):
    return local_call(toeplitz_kernel, jax.ShapeDtypeStruct((36 * CH, 2 * CH), BF16), [], 16, weight)


def spread_two(wide, base, saved, first, taps, out, at_out):
    positions = out.shape[1]
    stride = positions + 2 * ROW
    block = positions // 2
    for at in range(0, positions, block):
        lhs = jnp.concatenate(
            [
                wide[start : start + block, :]
                for frame in range(4)
                for q in range(3)
                for start in [(base + frame) * stride + at + (2 - q) * ROW]
            ],
            axis=1,
        )
        spread = jnp.dot(lhs, taps[...], preferred_element_type=F32)
        for j in range(2):
            value = saved[first + j, at : at + block, :].astype(F32)
            sigma = jax.nn.sigmoid(value)
            slope = sigma * (1.0 + value * (1.0 - sigma))
            out[at_out + j, at : at + block, :] = (spread[:, j * CH : (j + 1) * CH] * slope).astype(BF16)


def spread_mid(above, own, below, saved, taps, band, bands, following):
    positions = saved.shape[1]
    first = 2 if following else 0

    def kernel(band, above, own, below, saved, taps, *rest):
        out, wide, near = rest[-3:]
        frames = [with_rows(above, own, below, f, f, 2) for f in range(first, 4)]
        if following:
            frames += [next_frame(rest[0], rest[1], f, 2) for f in range(2)]
        store_frames(wide, frames)
        for j in range(2):
            near[j, 0:ROW, :] = above[first + j, 2 * ROW : 3 * ROW, :]
            near[j, ROW : ROW + positions, :] = saved[first + j]
            near[j, ROW + positions :, :] = below[first + j, 2 * ROW : 3 * ROW, :]
        spread_two(wide, 0, near, 0, taps, out, 0)

        def clear(at):
            for j in range(2):
                out[j, at : at + ROW, :] = jnp.zeros((ROW, CH), BF16)

        pl.when(band[0] == 0)(lambda: clear(0))
        pl.when(band[0] == bands - 1)(lambda: clear(ROW + positions))

    extended = (2, positions + 2 * ROW, CH)
    return local_call(
        kernel,
        jax.ShapeDtypeStruct(extended, BF16),
        [pltpu.VMEM((4 * (positions + 4 * ROW), 3 * CH), BF16), pltpu.VMEM(extended, BF16)],
        12,
        band, above, own, below, saved, taps, *following,
    )


def spread_all(low, high, later, saved, taps):
    def kernel(low, high, later, saved, taps, out, wide):
        store_frames(wide, [whole(ref, f) for ref in (low, high, later) for f in range(2)])
        spread_two(wide, 0, saved, 0, taps, out, 0)
        spread_two(wide, 2, saved, 2, taps, out, 2)

    return local_call(
        kernel,
        jax.ShapeDtypeStruct(saved.shape, BF16),
        [pltpu.VMEM((6 * low.shape[1], 3 * CH), BF16)],
        16,
        low, high, later, saved, taps,
    )


def store_share(out, total):
    planes, depth = out.shape[0], out.shape[1] // PAD
    chips = planes // 2
    share = 27 * CH // (2 * depth)
    for z in range(depth):
        for plane in range(planes):
            block, chip = 2 * z + plane // chips, plane % chips
            values = []
            for row in range(chip * PAD, (chip + 1) * PAD, 8):
                if row < share:
                    tap, line = divmod(block * share + row, CH)
                    p, tap = divmod(tap, 9)
                    values.append(total[p * CH + line : p * CH + line + 8, tap * CH : (tap + 1) * CH])
                else:
                    values.append(jnp.zeros((8, CH), F32))
            out[plane, z * PAD : (z + 1) * PAD, :] = jnp.concatenate(values).astype(BF16)


def store_acts(turned, saved, frames):
    for at, frame in enumerate(frames):
        value = saved[frame].astype(F32)
        turned[at * CH : (at + 1) * CH, :] = (value * jax.nn.sigmoid(value)).astype(BF16).T


def add_products(total, turned, wide, frames, first_frame, first_act, acts):
    positions = turned.shape[1]
    stride = positions + 2 * ROW
    for at in range(frames):
        frame = first_frame + at
        lowest = max(0, first_act - (frame - 2))
        top = min(2, first_act + acts - 1 - (frame - 2))
        s = frame - 2 + lowest - first_act
        rhs = jnp.concatenate(
            [
                wide[start : start + positions, :]
                for q in range(3)
                for start in [at * stride + (2 - q) * ROW]
            ],
            axis=1,
        )
        lhs = turned[s * CH : (s + top - lowest + 1) * CH, :]
        total[lowest * CH : (top + 1) * CH, :] += jnp.dot(lhs, rhs, preferred_element_type=F32)


TOTAL = (3 * CH, 9 * CH)


def sums(above, up, below, edges, later, saved_second, low, high, saved_first, planes, depth):
    positions = saved_first.shape[1]
    stride = positions + 2 * ROW

    def kernel(above, up, below, edges, later, s2, low, high, s1, share, partial, wide, acts, acts_first, total):
        store_acts(acts, s2, range(4))
        store_frames(wide, [with_rows(above, up, below, f, f, 1) for f in range(4)])
        store_frames(wide, [next_frame(edges, later, f, 1) for f in range(2)], 4)
        total[...] = jnp.zeros(TOTAL, F32)
        add_products(total, acts, wide, 6, 0, 0, 4)
        store_share(share, total)
        store_acts(acts_first, s1, range(4))
        store_frames(wide, [whole(ref, f) for ref in (low, high) for f in range(2)])
        partial[...] = jnp.zeros(TOTAL, F32)
        add_products(partial, acts_first, wide, 4, 0, 0, 4)

    return local_call(
        kernel,
        (
            jax.ShapeDtypeStruct((planes, depth * PAD, CH), BF16),
            jax.ShapeDtypeStruct(TOTAL, F32),
        ),
        [
            pltpu.VMEM((6 * stride, 3 * CH), BF16),
            pltpu.VMEM((4 * CH, positions), BF16),
            pltpu.VMEM((4 * CH, positions), BF16),
            pltpu.VMEM(TOTAL, F32),
        ],
        16,
        above, up, below, edges, later, saved_second, low, high, saved_first,
    )


def kept_and_sent(core, partial, later, saved_first, second):
    positions = saved_first.shape[1]

    def kernel(core, partial, later, saved, second, kept, sent, wide, acts, total):
        store_acts(acts, saved, (2, 3))
        store_frames(wide, [whole(later, f) for f in range(2)])
        total[...] = partial[...]
        add_products(total, acts, wide, 2, 4, 2, 2)

        def store(first_to, second_to):
            store_share(first_to, total)
            second_to[...] = second[...]

        pl.when(core[0] == 0)(lambda: store(kept, sent))
        pl.when(core[0] == 1)(lambda: store(sent, kept))

    out = jax.ShapeDtypeStruct(second.shape, BF16)
    return local_call(
        kernel,
        (out, out),
        [
            pltpu.VMEM((2 * later.shape[1], 3 * CH), BF16),
            pltpu.VMEM((2 * CH, positions), BF16),
            pltpu.VMEM(TOTAL, F32),
        ],
        12,
        core, partial, later, saved_first, second,
    )


def moved(block, axis, step):
    count = lax.axis_size(axis)
    route = [(i, i + step) for i in range(count) if 0 <= i + step < count]
    return lax.ppermute(block, axis, route)


def exchanged(pieces, axis):
    return lax.all_to_all(pieces, axis, split_axis=0, concat_axis=0, tiled=True)


def body(upstream, saved_first, saved_second, weight_first, weight_second):
    frames, height, width, chans = upstream.shape
    planes, depth = lax.axis_size(PLANE), lax.axis_size("z")
    flat = lambda a: a.reshape(frames, height * width, chans)
    up, s1, s2 = flat(upstream), flat(saved_first), flat(saved_second)

    band = lax.axis_index(ROWS).reshape(1)
    bands = lax.axis_size(ROWS)
    core = lax.axis_index("core").reshape(1)

    later = moved(up[:2], TM, -1)
    above = moved(jnp.concatenate([up[:, -2 * ROW :], s2[:, -ROW:]], axis=1), ROWS, 1)
    below = moved(jnp.concatenate([up[:, : 2 * ROW], s2[:, :ROW]], axis=1), ROWS, -1)
    edges = moved(jnp.concatenate([above[:2, : 2 * ROW], below[:2, : 2 * ROW]], axis=1), TM, -1)
    taps_second = toeplitz(weight_second)
    low = spread_mid(above, up, below, s2, taps_second, band, bands, ())
    mid_later = moved(low, TM, -1)
    taps_first = toeplitz(after(weight_first, low))
    high = spread_mid(
        above, up, below, after(s2, taps_first), taps_second, band, bands, (edges, later)
    )
    second, partial = sums(above, up, below, edges, later, s2, low, high, s1, planes, depth)
    kept, sent = kept_and_sent(core, partial, mid_later, s1, second)
    received = lax.ppermute(sent, "core", [(0, 1), (1, 0)])
    half = (kept.astype(F32) + received.astype(F32)).astype(BF16)
    part = exchanged(half, PLANE)
    part = part.astype(F32).sum(axis=0).astype(BF16)
    grad_input = spread_all(low, high, mid_later, s1, taps_first)
    part = exchanged(part.reshape(depth, PAD, CH), "z").astype(F32).sum(axis=0)
    factor = 1.0 / math.sqrt(
        frames * lax.axis_size(TM) * height * lax.axis_size(ROWS) * width
    )
    every = exchanged(jnp.broadcast_to(part * factor, (lax.axis_size(ROWS), PAD, CH)), ROWS)
    every = every.reshape(-1, 2, PAD, CH)
    share = weight_first.shape[0] // lax.axis_size(TM)
    share_first, share_second = (every[:, c].reshape(-1, CH)[:share] for c in range(2))
    return (grad_input.reshape(upstream.shape), share_first, share_second)


def solution(mesh):
    finer = Mesh(mesh.devices.reshape(8, 2, 2, 4, 2), ("z", "yh", "yl", "x", "core"))
    field = P(TM, ROWS, None, None)
    in_specs = (field, field, field, P(), P())
    out_specs = (field, P(TM, None), P(TM, None))
    return jax.shard_map(body, mesh=finer, in_specs=in_specs, out_specs=out_specs, check_vma=False)
```

```python
import math

import jax
import jax.numpy as jnp
from jax import lax
from jax.experimental import pallas as pl
from jax.experimental.pallas import tpu as pltpu
from jax.sharding import Mesh
from jax.sharding import PartitionSpec as P


TM = ("z", "yh")
PLANE = ("yh", "yl", "x")
ROWS = ("yl", "x", "core")
BF16 = jnp.bfloat16
F32 = jnp.float32
CH = 128


PAD = 32
BLOCK = 512
ROW = 128


def local_call(kernel, outs, scratch, mebibytes, *args, placed=()):
    specs = [pl.BlockSpec(memory_space=pl.ANY) if at in placed else pl.BlockSpec() for at in range(len(args))]
    return pl.pallas_call(
        kernel,
        out_shape=outs,
        in_specs=specs,
        scratch_shapes=scratch,
        compiler_params=pltpu.CompilerParams(vmem_limit_bytes=mebibytes * 1024 * 1024),
    )(*args)


def copied(parts, shapes, sources, space):
    def kernel(*refs):
        outs, sems = refs[len(sources) : -1], refs[-1]
        copies = [
            pltpu.make_async_copy(refs[source].at[at], outs[out].at[to], sems.at[n])
            for n, (out, to, source, at) in enumerate(parts)
        ]
        for copy in copies:
            copy.start()
        for copy in copies:
            copy.wait()

    return pl.pallas_call(
        kernel,
        out_shape=[jax.ShapeDtypeStruct(shape, sources[0].dtype) for shape in shapes],
        in_specs=[pl.BlockSpec(memory_space=space)] * len(sources),
        scratch_shapes=[pltpu.SemaphoreType.DMA((len(parts),))],
        compiler_params=pltpu.CompilerParams(vmem_limit_bytes=8 * 1024 * 1024),
    )(*sources)


def rows_of(frames, begin, size):
    return (slice(0, frames), slice(begin, begin + size))


def added(own, other):
    def kernel(own, other, out):
        for at in range(out.shape[0]):
            out[at] = (own[at].astype(F32) + other[at].astype(F32)).astype(BF16)

    return local_call(kernel, jax.ShapeDtypeStruct(own.shape, BF16), [], 8, own, other)


def summed_copies(pieces, copies, factor):
    def kernel(pieces, out):
        total = pieces[0].astype(F32)
        for at in range(1, pieces.shape[0]):
            total += pieces[at].astype(F32)
        for at in range(copies):
            out[at] = total * factor

    out = jax.ShapeDtypeStruct((copies, *pieces.shape[1:]), F32)
    return local_call(kernel, out, [], 8, pieces)


def shares(every, share):
    def kernel(every, first, second):
        for out, core in ((first, 0), (second, 1)):
            for chip in range(every.shape[0] // 2):
                rows = min(PAD, share - chip * PAD)
                if rows > 0:
                    out[chip * PAD : chip * PAD + rows, :] = every[2 * chip + core, 0:rows, :]

    out = jax.ShapeDtypeStruct((share, CH), F32)
    return local_call(kernel, (out, out), [], 8, every)


def store_shifted(dest, base, part):
    size = part.shape[0]
    wide = part.astype(F32)
    column = lax.broadcasted_iota(jnp.int32, (size, CH), 0) % 128
    later = jnp.where(column == 127, 0.0, pltpu.roll(wide, size - 1, 0))
    before = jnp.where(column == 0, 0.0, pltpu.roll(wide, 1, 0))
    dest[base : base + size, 0:CH] = later.astype(BF16)
    dest[base : base + size, CH : 2 * CH] = part
    dest[base : base + size, 2 * CH : 3 * CH] = before.astype(BF16)


def with_rows(above, own, below, frame, at, rows):
    size = rows * ROW
    return [
        (above, frame, 2 * ROW - size, size),
        (own, at, 0, own.shape[1]),
        (below, frame, 0, size),
    ]


def next_frame(edges, own, frame, rows):
    size = rows * ROW
    return [
        (edges, frame, 2 * ROW - size, size),
        (own, frame, 0, own.shape[1]),
        (edges, frame, 2 * ROW, size),
    ]


def whole(ref, frame):
    return [(ref, frame, 0, ref.shape[1])]


def store_frames(dest, frames, first=0):
    stride = sum(piece[3] for piece in frames[0])
    for frame, pieces in enumerate(frames):
        base = (first + frame) * stride
        for ref, at, begin, rows in pieces:
            step = min(rows, 256)
            for start in range(begin, begin + rows, step):
                store_shifted(dest, base, ref[at, start : start + step])
                base += step


def toeplitz_kernel(weight, out):
    zero = jnp.zeros((CH, CH), BF16)
    for tap in range(9):
        for p in range(3):
            at = (9 * p + tap) * CH
            turned = weight[at : at + CH, :].T
            for j in range(2):
                row = (9 * (j + 2 - p) + tap) * CH
                out[row : row + CH, j * CH : (j + 1) * CH] = turned
        out[(27 + tap) * CH : (28 + tap) * CH, 0:CH] = zero
        out[tap * CH : (tap + 1) * CH, CH : 2 * CH] = zero


def toeplitz(weight):
    return local_call(toeplitz_kernel, jax.ShapeDtypeStruct((36 * CH, 2 * CH), BF16), [], 16, weight)


def spread_two(wide, base, saved, first, taps, out, at_out):
    positions = out.shape[1]
    stride = positions + 2 * ROW
    for at in range(0, positions, BLOCK):
        block = min(BLOCK, positions - at)
        lhs = jnp.concatenate(
            [
                wide[start : start + block, :]
                for frame in range(4)
                for q in range(3)
                for start in [(base + frame) * stride + at + (2 - q) * ROW]
            ],
            axis=1,
        )
        spread = jnp.dot(lhs, taps[...], preferred_element_type=F32)
        for j in range(2):
            value = saved[first + j, at : at + block, :].astype(F32)
            sigma = jax.nn.sigmoid(value)
            slope = sigma * (1.0 + value * (1.0 - sigma))
            out[at_out + j, at : at + block, :] = (spread[:, j * CH : (j + 1) * CH] * slope).astype(BF16)


def spread_mid(above, own, below, saved, taps, bands, following):
    positions = saved.shape[1]
    first = 2 if following else 0

    def kernel(above, own, below, saved, taps, *rest):
        out, wide, near, sem = rest[-4:]
        inner = near.at[:, ROW : ROW + positions, :]
        copy = pltpu.make_async_copy(saved.at[first : first + 2], inner, sem)
        copy.start()
        frames = [with_rows(above, own, below, f, f, 2) for f in range(first, 4)]
        if following:
            frames += [next_frame(rest[0], rest[1], f, 2) for f in range(2)]
        store_frames(wide, frames)
        for j in range(2):
            near[j, 0:ROW, :] = above[first + j, 2 * ROW : 3 * ROW, :]
            near[j, ROW + positions :, :] = below[first + j, 2 * ROW : 3 * ROW, :]
        copy.wait()
        spread_two(wide, 0, near, 0, taps, out, 0)

        def clear(at):
            for j in range(2):
                out[j, at : at + ROW, :] = jnp.zeros((ROW, CH), BF16)

        band = lax.axis_index(ROWS)
        pl.when(band == 0)(lambda: clear(0))
        pl.when(band == bands - 1)(lambda: clear(ROW + positions))

    extended = (2, positions + 2 * ROW, CH)
    return local_call(
        kernel,
        jax.ShapeDtypeStruct(extended, BF16),
        [
            pltpu.VMEM((4 * (positions + 4 * ROW), 3 * CH), BF16),
            pltpu.VMEM(extended, BF16),
            pltpu.SemaphoreType.DMA,
        ],
        12,
        above, own, below, saved, taps, *following,
        placed=(3,),
    )


def spread_all(low, high, later, saved, weight):
    def kernel(low, high, later, saved, weight, out, wide, taps):
        toeplitz_kernel(weight, taps)
        store_frames(wide, [whole(ref, f) for ref in (low, high, later) for f in range(2)])
        spread_two(wide, 0, saved, 0, taps, out, 0)
        spread_two(wide, 2, saved, 2, taps, out, 2)

    return local_call(
        kernel,
        jax.ShapeDtypeStruct(saved.shape, BF16),
        [pltpu.VMEM((6 * low.shape[1], 3 * CH), BF16), pltpu.VMEM((36 * CH, 2 * CH), BF16)],
        18,
        low, high, later, saved, weight,
    )


def store_share(out, total):
    planes, depth = out.shape[0], out.shape[1] // PAD
    chips = planes // 2
    share = 27 * CH // (2 * depth)
    for z in range(depth):
        for plane in range(planes):
            block, chip = 2 * z + plane // chips, plane % chips
            values = []
            for row in range(chip * PAD, (chip + 1) * PAD, 8):
                if row < share:
                    tap, line = divmod(block * share + row, CH)
                    p, tap = divmod(tap, 9)
                    values.append(total[p * CH + line : p * CH + line + 8, tap * CH : (tap + 1) * CH])
                else:
                    values.append(jnp.zeros((8, CH), F32))
            out[plane, z * PAD : (z + 1) * PAD, :] = jnp.concatenate(values).astype(BF16)


def store_acts(turned, saved, frames):
    for at, frame in enumerate(frames):
        value = saved[frame].astype(F32)
        turned[at * CH : (at + 1) * CH, :] = (value * jax.nn.sigmoid(value)).astype(BF16).T


def add_products(total, turned, wide, frames, first_frame, first_act, acts):
    positions = turned.shape[1]
    stride = positions + 2 * ROW
    for at in range(frames):
        frame = first_frame + at
        lowest = max(0, first_act - (frame - 2))
        top = min(2, first_act + acts - 1 - (frame - 2))
        s = frame - 2 + lowest - first_act
        rhs = jnp.concatenate(
            [
                wide[start : start + positions, :]
                for q in range(3)
                for start in [at * stride + (2 - q) * ROW]
            ],
            axis=1,
        )
        lhs = turned[s * CH : (s + top - lowest + 1) * CH, :]
        total[lowest * CH : (top + 1) * CH, :] += jnp.dot(lhs, rhs, preferred_element_type=F32)


TOTAL = (3 * CH, 9 * CH)


def sums(above, up, below, edges, later, saved_second, low, high, saved_first, planes, depth):
    positions = saved_first.shape[1]
    stride = positions + 2 * ROW

    def kernel(above, up, below, edges, later, s2, low, high, s1, share, partial, wide, acts, acts_first, total):
        store_acts(acts, s2, range(4))
        store_frames(wide, [with_rows(above, up, below, f, f, 1) for f in range(4)])
        store_frames(wide, [next_frame(edges, later, f, 1) for f in range(2)], 4)
        total[...] = jnp.zeros(TOTAL, F32)
        add_products(total, acts, wide, 6, 0, 0, 4)
        store_share(share, total)
        store_acts(acts_first, s1, range(4))
        store_frames(wide, [whole(ref, f) for ref in (low, high) for f in range(2)])
        partial[...] = jnp.zeros(TOTAL, F32)
        add_products(partial, acts_first, wide, 4, 0, 0, 4)

    return local_call(
        kernel,
        (
            jax.ShapeDtypeStruct((planes, depth * PAD, CH), BF16),
            jax.ShapeDtypeStruct(TOTAL, F32),
        ),
        [
            pltpu.VMEM((6 * stride, 3 * CH), BF16),
            pltpu.VMEM((4 * CH, positions), BF16),
            pltpu.VMEM((4 * CH, positions), BF16),
            pltpu.VMEM(TOTAL, F32),
        ],
        16,
        above, up, below, edges, later, saved_second, low, high, saved_first,
    )


def kept_and_sent(partial, later, saved_first, second):
    positions = saved_first.shape[1]

    def kernel(partial, later, saved, second, kept, sent, wide, acts, total):
        store_acts(acts, saved, (2, 3))
        store_frames(wide, [whole(later, f) for f in range(2)])
        total[...] = partial[...]
        add_products(total, acts, wide, 2, 4, 2, 2)

        def store(first_to, second_to):
            store_share(first_to, total)
            second_to[...] = second[...]

        core = lax.axis_index("core")
        pl.when(core == 0)(lambda: store(kept, sent))
        pl.when(core == 1)(lambda: store(sent, kept))

    out = jax.ShapeDtypeStruct(second.shape, BF16)
    return local_call(
        kernel,
        (out, out),
        [
            pltpu.VMEM((2 * later.shape[1], 3 * CH), BF16),
            pltpu.VMEM((2 * CH, positions), BF16),
            pltpu.VMEM(TOTAL, F32),
        ],
        12,
        partial, later, saved_first, second,
    )


def moved(block, axis, step):
    count = lax.axis_size(axis)
    route = [(i, i + step) for i in range(count) if 0 <= i + step < count]
    return lax.ppermute(block, axis, route)


def exchanged(pieces, axis):
    return lax.all_to_all(pieces, axis, split_axis=0, concat_axis=0, tiled=True)


def body(upstream, saved_first, saved_second, weight_first, weight_second):
    frames, height, width, chans = upstream.shape
    planes, depth = lax.axis_size(PLANE), lax.axis_size("z")
    flat = lambda a: a.reshape(frames, height * width, chans)
    up, s1, s2 = flat(upstream), flat(saved_first), flat(saved_second)

    bands = lax.axis_size(ROWS)

    size = up.shape[1]
    tail, head, start, up_near, s2_near = copied(
        (
            (0, rows_of(4, 0, 2 * ROW), 0, rows_of(4, size - 2 * ROW, 2 * ROW)),
            (0, rows_of(4, 2 * ROW, ROW), 1, rows_of(4, size - ROW, ROW)),
            (1, rows_of(4, 0, 2 * ROW), 0, rows_of(4, 0, 2 * ROW)),
            (1, rows_of(4, 2 * ROW, ROW), 1, rows_of(4, 0, ROW)),
            (2, rows_of(2, 0, size), 0, rows_of(2, 0, size)),
            (3, rows_of(4, 0, size), 0, rows_of(4, 0, size)),
            (4, rows_of(4, 0, size), 1, rows_of(4, 0, size)),
        ),
        ((frames, 3 * ROW, CH), (frames, 3 * ROW, CH), (2, size, CH), up.shape, up.shape),
        tuple(pltpu.with_memory_space_constraint(a, pltpu.HBM) for a in (up, s2)),
        pltpu.HBM,
    )
    above = moved(tail, ROWS, 1)
    below = moved(head, ROWS, -1)
    later = moved(start, TM, -1)
    (packed,) = copied(
        (
            (0, rows_of(2, 0, 2 * ROW), 0, rows_of(2, 0, 2 * ROW)),
            (0, rows_of(2, 2 * ROW, 2 * ROW), 1, rows_of(2, 0, 2 * ROW)),
        ),
        ((2, 4 * ROW, CH),),
        (above, below),
        pl.ANY,
    )
    edges = moved(packed, TM, -1)
    taps_second = toeplitz(weight_second)
    low = spread_mid(above, up_near, below, s2_near, taps_second, bands, ())
    mid_later = moved(low, TM, -1)
    high = spread_mid(
        above, up_near, below, s2_near, taps_second, bands, (edges, later)
    )
    second, partial = sums(above, up_near, below, edges, later, s2_near, low, high, s1, planes, depth)
    kept, sent = kept_and_sent(partial, mid_later, s1, second)
    received = lax.ppermute(sent, "core", [(0, 1), (1, 0)])
    half = added(kept, received)
    part = exchanged(half, PLANE)
    part = part.astype(F32).sum(axis=0).astype(BF16)
    grad_input = spread_all(low, high, mid_later, s1, weight_first)
    part = exchanged(part.reshape(depth, PAD, CH), "z")
    factor = 1.0 / math.sqrt(frames * lax.axis_size(TM) * height * bands * width)
    every = exchanged(summed_copies(part, bands, factor), ROWS)
    share_first, share_second = shares(every, weight_first.shape[0] // lax.axis_size(TM))
    return (grad_input.reshape(upstream.shape), share_first, share_second)


def solution(mesh):
    finer = Mesh(mesh.devices.reshape(8, 2, 2, 4, 2), ("z", "yh", "yl", "x", "core"))
    field = P(TM, ROWS, None, None)
    in_specs = (field, field, field, P(), P())
    out_specs = (field, P(TM, None), P(TM, None))
    return jax.shard_map(body, mesh=finer, in_specs=in_specs, out_specs=out_specs, check_vma=False)
```

```python
import math

import jax
import jax.numpy as jnp
from jax import lax
from jax.experimental import pallas as pl
from jax.experimental.pallas import tpu as pltpu
from jax.sharding import Mesh
from jax.sharding import PartitionSpec as P


TM = ("z", "yh")
PLANE = ("yh", "yl", "x")
ROWS = ("yl", "x", "core")
BF16 = jnp.bfloat16
F32 = jnp.float32
CH = 128


PAD = 32
BLOCK = 512
ROW = 128


def local_call(kernel, outs, scratch, mebibytes, *args, placed=()):
    specs = [pl.BlockSpec(memory_space=pl.ANY) if at in placed else pl.BlockSpec() for at in range(len(args))]
    return pl.pallas_call(
        kernel,
        out_shape=outs,
        in_specs=specs,
        scratch_shapes=scratch,
        compiler_params=pltpu.CompilerParams(vmem_limit_bytes=mebibytes * 1024 * 1024),
    )(*args)


def copied(parts, shapes, sources, space):
    def kernel(*refs):
        outs, sems = refs[len(sources) : -1], refs[-1]
        copies = [
            pltpu.make_async_copy(refs[source].at[at], outs[out].at[to], sems.at[n])
            for n, (out, to, source, at) in enumerate(parts)
        ]
        for copy in copies:
            copy.start()
        for copy in copies:
            copy.wait()

    return pl.pallas_call(
        kernel,
        out_shape=[jax.ShapeDtypeStruct(shape, sources[0].dtype) for shape in shapes],
        in_specs=[pl.BlockSpec(memory_space=space)] * len(sources),
        scratch_shapes=[pltpu.SemaphoreType.DMA((len(parts),))],
        compiler_params=pltpu.CompilerParams(vmem_limit_bytes=8 * 1024 * 1024),
    )(*sources)


def rows_of(frames, begin, size):
    return (slice(0, frames), slice(begin, begin + size))


def added(own, other):
    def kernel(own, other, out):
        for at in range(out.shape[0]):
            out[at] = (own[at].astype(F32) + other[at].astype(F32)).astype(BF16)

    return local_call(kernel, jax.ShapeDtypeStruct(own.shape, BF16), [], 8, own, other)


def summed_copies(pieces, copies, factor):
    def kernel(pieces, out):
        total = pieces[0].astype(F32)
        for at in range(1, pieces.shape[0]):
            total += pieces[at].astype(F32)
        for at in range(copies):
            out[at] = total * factor

    out = jax.ShapeDtypeStruct((copies, *pieces.shape[1:]), F32)
    return local_call(kernel, out, [], 8, pieces)


def shares(every, share):
    def kernel(every, first, second):
        for out, core in ((first, 0), (second, 1)):
            for chip in range(every.shape[0] // 2):
                rows = min(PAD, share - chip * PAD)
                if rows > 0:
                    out[chip * PAD : chip * PAD + rows, :] = every[2 * chip + core, 0:rows, :]

    out = jax.ShapeDtypeStruct((share, CH), F32)
    return local_call(kernel, (out, out), [], 8, every)


def store_shifted(dest, base, part):
    size = part.shape[0]
    wide = part.astype(F32)
    column = lax.broadcasted_iota(jnp.int32, (size, CH), 0) % 128
    later = jnp.where(column == 127, 0.0, pltpu.roll(wide, size - 1, 0))
    before = jnp.where(column == 0, 0.0, pltpu.roll(wide, 1, 0))
    dest[base : base + size, 0:CH] = later.astype(BF16)
    dest[base : base + size, CH : 2 * CH] = part
    dest[base : base + size, 2 * CH : 3 * CH] = before.astype(BF16)


def with_rows(above, own, below, frame, at, rows):
    size = rows * ROW
    return [
        (above, frame, 2 * ROW - size, size),
        (own, at, 0, own.shape[1]),
        (below, frame, 0, size),
    ]


def next_frame(edges, own, frame, rows):
    size = rows * ROW
    return [
        (edges, frame, 2 * ROW - size, size),
        (own, frame, 0, own.shape[1]),
        (edges, frame, 2 * ROW, size),
    ]


def whole(ref, frame):
    return [(ref, frame, 0, ref.shape[1])]


def store_frames(dest, frames, first=0):
    stride = sum(piece[3] for piece in frames[0])
    for frame, pieces in enumerate(frames):
        base = (first + frame) * stride
        for ref, at, begin, rows in pieces:
            step = min(rows, 256)
            for start in range(begin, begin + rows, step):
                store_shifted(dest, base, ref[at, start : start + step])
                base += step


def toeplitz_kernel(weight, out):
    zero = jnp.zeros((CH, CH), BF16)
    for tap in range(9):
        for p in range(3):
            at = (9 * p + tap) * CH
            turned = weight[at : at + CH, :].T
            for j in range(2):
                row = (9 * (j + 2 - p) + tap) * CH
                out[row : row + CH, j * CH : (j + 1) * CH] = turned
        out[(27 + tap) * CH : (28 + tap) * CH, 0:CH] = zero
        out[tap * CH : (tap + 1) * CH, CH : 2 * CH] = zero


def toeplitz(weight):
    return local_call(toeplitz_kernel, jax.ShapeDtypeStruct((36 * CH, 2 * CH), BF16), [], 16, weight)


def spread_two(wide, base, saved, first, taps, out, at_out):
    positions = out.shape[1]
    stride = positions + 2 * ROW
    for at in range(0, positions, BLOCK):
        block = min(BLOCK, positions - at)
        lhs = jnp.concatenate(
            [
                wide[start : start + block, :]
                for frame in range(4)
                for q in range(3)
                for start in [(base + frame) * stride + at + (2 - q) * ROW]
            ],
            axis=1,
        )
        spread = jnp.dot(lhs, taps[...], preferred_element_type=F32)
        for j in range(2):
            value = saved[first + j, at : at + block, :].astype(F32)
            sigma = jax.nn.sigmoid(value)
            slope = sigma * (1.0 + value * (1.0 - sigma))
            out[at_out + j, at : at + block, :] = (spread[:, j * CH : (j + 1) * CH] * slope).astype(BF16)


def spread_mid(above, own, below, saved, taps, bands, following):
    positions = saved.shape[1]
    first = 2 if following else 0

    def kernel(above, own, below, saved, taps, *rest):
        out, wide, near, sem = rest[-4:]
        inner = near.at[:, ROW : ROW + positions, :]
        copy = pltpu.make_async_copy(saved.at[first : first + 2], inner, sem)
        copy.start()
        frames = [with_rows(above, own, below, f, f, 2) for f in range(first, 4)]
        if following:
            frames += [next_frame(rest[0], rest[1], f, 2) for f in range(2)]
        store_frames(wide, frames)
        for j in range(2):
            near[j, 0:ROW, :] = above[first + j, 2 * ROW : 3 * ROW, :]
            near[j, ROW + positions :, :] = below[first + j, 2 * ROW : 3 * ROW, :]
        copy.wait()
        spread_two(wide, 0, near, 0, taps, out, 0)

        def clear(at):
            for j in range(2):
                out[j, at : at + ROW, :] = jnp.zeros((ROW, CH), BF16)

        band = lax.axis_index(ROWS)
        pl.when(band == 0)(lambda: clear(0))
        pl.when(band == bands - 1)(lambda: clear(ROW + positions))

    extended = (2, positions + 2 * ROW, CH)
    return local_call(
        kernel,
        jax.ShapeDtypeStruct(extended, BF16),
        [
            pltpu.VMEM((4 * (positions + 4 * ROW), 3 * CH), BF16),
            pltpu.VMEM(extended, BF16),
            pltpu.SemaphoreType.DMA,
        ],
        12,
        above, own, below, saved, taps, *following,
        placed=(3,),
    )


def spread_all(low, high, later, saved, weight):
    def kernel(low, high, later, saved, weight, out, wide, taps):
        toeplitz_kernel(weight, taps)
        store_frames(wide, [whole(ref, f) for ref in (low, high, later) for f in range(2)])
        spread_two(wide, 0, saved, 0, taps, out, 0)
        spread_two(wide, 2, saved, 2, taps, out, 2)

    return local_call(
        kernel,
        jax.ShapeDtypeStruct(saved.shape, BF16),
        [pltpu.VMEM((6 * low.shape[1], 3 * CH), BF16), pltpu.VMEM((36 * CH, 2 * CH), BF16)],
        18,
        low, high, later, saved, weight,
    )


def store_share(out, total):
    planes, depth = out.shape[0], out.shape[1] // PAD
    chips = planes // 2
    share = 27 * CH // (2 * depth)
    for z in range(depth):
        for plane in range(planes):
            block, chip = 2 * z + plane // chips, plane % chips
            values = []
            for row in range(chip * PAD, (chip + 1) * PAD, 8):
                if row < share:
                    tap, line = divmod(block * share + row, CH)
                    p, tap = divmod(tap, 9)
                    values.append(total[p * CH + line : p * CH + line + 8, tap * CH : (tap + 1) * CH])
                else:
                    values.append(jnp.zeros((8, CH), F32))
            out[plane, z * PAD : (z + 1) * PAD, :] = jnp.concatenate(values).astype(BF16)


def store_acts(turned, saved, frames):
    for at, frame in enumerate(frames):
        value = saved[frame].astype(F32)
        turned[at * CH : (at + 1) * CH, :] = (value * jax.nn.sigmoid(value)).astype(BF16).T


def add_products(total, turned, wide, frames, first_frame, first_act, acts):
    positions = turned.shape[1]
    stride = positions + 2 * ROW
    for at in range(frames):
        frame = first_frame + at
        lowest = max(0, first_act - (frame - 2))
        top = min(2, first_act + acts - 1 - (frame - 2))
        s = frame - 2 + lowest - first_act
        rhs = jnp.concatenate(
            [
                wide[start : start + positions, :]
                for q in range(3)
                for start in [at * stride + (2 - q) * ROW]
            ],
            axis=1,
        )
        lhs = turned[s * CH : (s + top - lowest + 1) * CH, :]
        total[lowest * CH : (top + 1) * CH, :] += jnp.dot(lhs, rhs, preferred_element_type=F32)


TOTAL = (3 * CH, 9 * CH)


def sum_here(above, up, below, saved):
    positions = saved.shape[1]

    def kernel(above, up, below, saved, total, wide, acts):
        store_acts(acts, saved, range(4))
        store_frames(wide, [with_rows(above, up, below, f, f, 1) for f in range(4)])
        total[...] = jnp.zeros(TOTAL, F32)
        add_products(total, acts, wide, 4, 0, 0, 4)

    return local_call(
        kernel,
        jax.ShapeDtypeStruct(TOTAL, F32),
        [
            pltpu.VMEM((4 * (positions + 2 * ROW), 3 * CH), BF16),
            pltpu.VMEM((4 * CH, positions), BF16),
        ],
        14,
        above, up, below, saved,
    )


def sums(here, edges, later, saved_second, low, high, saved_first, planes, depth):
    positions = saved_first.shape[1]

    def kernel(here, edges, later, s2, low, high, s1, share, partial, wide, near, acts, acts_first, total):
        store_acts(acts, s2, (2, 3))
        store_frames(near, [next_frame(edges, later, f, 1) for f in range(2)])
        total[...] = here[...]
        add_products(total, acts, near, 2, 4, 2, 2)
        store_share(share, total)
        store_acts(acts_first, s1, range(4))
        store_frames(wide, [whole(ref, f) for ref in (low, high) for f in range(2)])
        partial[...] = jnp.zeros(TOTAL, F32)
        add_products(partial, acts_first, wide, 4, 0, 0, 4)

    return local_call(
        kernel,
        (
            jax.ShapeDtypeStruct((planes, depth * PAD, CH), BF16),
            jax.ShapeDtypeStruct(TOTAL, F32),
        ),
        [
            pltpu.VMEM((4 * low.shape[1], 3 * CH), BF16),
            pltpu.VMEM((2 * low.shape[1], 3 * CH), BF16),
            pltpu.VMEM((2 * CH, positions), BF16),
            pltpu.VMEM((4 * CH, positions), BF16),
            pltpu.VMEM(TOTAL, F32),
        ],
        18,
        here, edges, later, saved_second, low, high, saved_first,
    )


def kept_and_sent(partial, later, saved_first, second):
    positions = saved_first.shape[1]

    def kernel(partial, later, saved, second, kept, sent, wide, acts, total):
        store_acts(acts, saved, (2, 3))
        store_frames(wide, [whole(later, f) for f in range(2)])
        total[...] = partial[...]
        add_products(total, acts, wide, 2, 4, 2, 2)

        def store(first_to, second_to):
            store_share(first_to, total)
            second_to[...] = second[...]

        core = lax.axis_index("core")
        pl.when(core == 0)(lambda: store(kept, sent))
        pl.when(core == 1)(lambda: store(sent, kept))

    out = jax.ShapeDtypeStruct(second.shape, BF16)
    return local_call(
        kernel,
        (out, out),
        [
            pltpu.VMEM((2 * later.shape[1], 3 * CH), BF16),
            pltpu.VMEM((2 * CH, positions), BF16),
            pltpu.VMEM(TOTAL, F32),
        ],
        12,
        partial, later, saved_first, second,
    )


def moved(block, axis, step):
    count = lax.axis_size(axis)
    route = [(i, i + step) for i in range(count) if 0 <= i + step < count]
    return lax.ppermute(block, axis, route)


def exchanged(pieces, axis):
    return lax.all_to_all(pieces, axis, split_axis=0, concat_axis=0, tiled=True)


def body(upstream, saved_first, saved_second, weight_first, weight_second):
    frames, height, width, chans = upstream.shape
    planes, depth = lax.axis_size(PLANE), lax.axis_size("z")
    flat = lambda a: a.reshape(frames, height * width, chans)
    up, s1, s2 = flat(upstream), flat(saved_first), flat(saved_second)

    bands = lax.axis_size(ROWS)

    size = up.shape[1]
    tail, head, start, up_near, s2_near = copied(
        (
            (0, rows_of(4, 0, 2 * ROW), 0, rows_of(4, size - 2 * ROW, 2 * ROW)),
            (0, rows_of(4, 2 * ROW, ROW), 1, rows_of(4, size - ROW, ROW)),
            (1, rows_of(4, 0, 2 * ROW), 0, rows_of(4, 0, 2 * ROW)),
            (1, rows_of(4, 2 * ROW, ROW), 1, rows_of(4, 0, ROW)),
            (2, rows_of(2, 0, size), 0, rows_of(2, 0, size)),
            (3, rows_of(4, 0, size), 0, rows_of(4, 0, size)),
            (4, rows_of(4, 0, size), 1, rows_of(4, 0, size)),
        ),
        ((frames, 3 * ROW, CH), (frames, 3 * ROW, CH), (2, size, CH), up.shape, up.shape),
        tuple(pltpu.with_memory_space_constraint(a, pltpu.HBM) for a in (up, s2)),
        pltpu.HBM,
    )
    above = moved(tail, ROWS, 1)
    below = moved(head, ROWS, -1)
    later = moved(start, TM, -1)
    (packed,) = copied(
        (
            (0, rows_of(2, 0, 2 * ROW), 0, rows_of(2, 0, 2 * ROW)),
            (0, rows_of(2, 2 * ROW, 2 * ROW), 1, rows_of(2, 0, 2 * ROW)),
        ),
        ((2, 4 * ROW, CH),),
        (above, below),
        pl.ANY,
    )
    edges = moved(packed, TM, -1)
    taps_second = toeplitz(weight_second)
    low = spread_mid(above, up_near, below, s2_near, taps_second, bands, ())
    mid_later = moved(low, TM, -1)
    here = sum_here(above, up_near, below, s2_near)
    high = spread_mid(
        above, up_near, below, s2_near, taps_second, bands, (edges, later)
    )
    second, partial = sums(here, edges, later, s2_near, low, high, s1, planes, depth)
    kept, sent = kept_and_sent(partial, mid_later, s1, second)
    received = lax.ppermute(sent, "core", [(0, 1), (1, 0)])
    half = added(kept, received)
    part = exchanged(half, PLANE)
    part = part.astype(F32).sum(axis=0).astype(BF16)
    grad_input = spread_all(low, high, mid_later, s1, weight_first)
    part = exchanged(part.reshape(depth, PAD, CH), "z")
    factor = 1.0 / math.sqrt(frames * lax.axis_size(TM) * height * bands * width)
    every = exchanged(summed_copies(part, bands, factor), ROWS)
    share_first, share_second = shares(every, weight_first.shape[0] // lax.axis_size(TM))
    return (grad_input.reshape(upstream.shape), share_first, share_second)


def solution(mesh):
    finer = Mesh(mesh.devices.reshape(8, 2, 2, 4, 2), ("z", "yh", "yl", "x", "core"))
    field = P(TM, ROWS, None, None)
    in_specs = (field, field, field, P(), P())
    out_specs = (field, P(TM, None), P(TM, None))
    return jax.shard_map(body, mesh=finer, in_specs=in_specs, out_specs=out_specs, check_vma=False)
```

```python
import math

import jax
import jax.numpy as jnp
from jax import lax
from jax.experimental import pallas as pl
from jax.experimental.pallas import tpu as pltpu
from jax.sharding import Mesh
from jax.sharding import PartitionSpec as P


TM = ("z", "yh")
PLANE = ("yh", "yl", "x")
ROWS = ("yl", "x", "core")
BF16 = jnp.bfloat16
F32 = jnp.float32
CH = 128


TILE = 8
SLOTS = 4
BLOCK = 512
ROW = 128


def local_call(kernel, outs, scratch, mebibytes, *args, placed=()):
    specs = [pl.BlockSpec(memory_space=pl.ANY) if at in placed else pl.BlockSpec() for at in range(len(args))]
    return pl.pallas_call(
        kernel,
        out_shape=outs,
        in_specs=specs,
        scratch_shapes=scratch,
        compiler_params=pltpu.CompilerParams(vmem_limit_bytes=mebibytes * 1024 * 1024),
    )(*args)


def copied(parts, shapes, sources, space):
    def kernel(*refs):
        outs, sems = refs[len(sources) : -1], refs[-1]
        copies = [
            pltpu.make_async_copy(refs[source].at[at], outs[out].at[to], sems.at[n])
            for n, (out, to, source, at) in enumerate(parts)
        ]
        for copy in copies:
            copy.start()
        for copy in copies:
            copy.wait()

    return pl.pallas_call(
        kernel,
        out_shape=[jax.ShapeDtypeStruct(shape, sources[0].dtype) for shape in shapes],
        in_specs=[pl.BlockSpec(memory_space=space)] * len(sources),
        scratch_shapes=[pltpu.SemaphoreType.DMA((len(parts),))],
        compiler_params=pltpu.CompilerParams(vmem_limit_bytes=8 * 1024 * 1024),
    )(*sources)


def rows_of(frames, begin, size):
    return (slice(0, frames), slice(begin, begin + size))


def added(own, other):
    def kernel(own, other, out):
        for at in range(out.shape[0]):
            out[at] = (own[at].astype(F32) + other[at].astype(F32)).astype(BF16)

    return local_call(kernel, jax.ShapeDtypeStruct(own.shape, BF16), [], 8, own, other)


def summed_copies(pieces, copies, factor):
    def kernel(pieces, out):
        total = pieces[0].astype(F32)
        for at in range(1, pieces.shape[0]):
            total += pieces[at].astype(F32)
        for at in range(copies):
            out[at] = total * factor

    out = jax.ShapeDtypeStruct((copies, *pieces.shape[1:]), F32)
    return local_call(kernel, out, [], 8, pieces)


def shares(every, share):
    chips, tiles = every.shape[0] // 2, share // TILE

    def kernel(every, first, second):
        z = lax.axis_index("z")
        for k in range(tiles):
            chip = lax.rem(tiles * z + k, chips)
            rows = slice(k * TILE, (k + 1) * TILE)
            first[rows, :] = every[2 * chip, k // chips]
            second[rows, :] = every[2 * chip + 1, k // chips]

    out = jax.ShapeDtypeStruct((share, CH), F32)
    return local_call(kernel, (out, out), [], 8, every)


def store_shifted(dest, base, part):
    size = part.shape[0]
    wide = part.astype(F32)
    column = lax.broadcasted_iota(jnp.int32, (size, CH), 0) % 128
    later = jnp.where(column == 127, 0.0, pltpu.roll(wide, size - 1, 0))
    before = jnp.where(column == 0, 0.0, pltpu.roll(wide, 1, 0))
    dest[base : base + size, 0:CH] = later.astype(BF16)
    dest[base : base + size, CH : 2 * CH] = part
    dest[base : base + size, 2 * CH : 3 * CH] = before.astype(BF16)


def with_rows(above, own, below, frame, at, rows):
    size = rows * ROW
    return [
        (above, frame, 2 * ROW - size, size),
        (own, at, 0, own.shape[1]),
        (below, frame, 0, size),
    ]


def next_frame(edges, own, frame, rows):
    size = rows * ROW
    return [
        (edges, frame, 2 * ROW - size, size),
        (own, frame, 0, own.shape[1]),
        (edges, frame, 2 * ROW, size),
    ]


def whole(ref, frame):
    return [(ref, frame, 0, ref.shape[1])]


def store_frames(dest, frames, first=0):
    stride = sum(piece[3] for piece in frames[0])
    for frame, pieces in enumerate(frames):
        base = (first + frame) * stride
        for ref, at, begin, rows in pieces:
            step = min(rows, 256)
            for start in range(begin, begin + rows, step):
                store_shifted(dest, base, ref[at, start : start + step])
                base += step


def toeplitz_kernel(weight, out):
    zero = jnp.zeros((CH, CH), BF16)
    for tap in range(9):
        for p in range(3):
            at = (9 * p + tap) * CH
            turned = weight[at : at + CH, :].T
            for j in range(2):
                row = (9 * (j + 2 - p) + tap) * CH
                out[row : row + CH, j * CH : (j + 1) * CH] = turned
        out[(27 + tap) * CH : (28 + tap) * CH, 0:CH] = zero
        out[tap * CH : (tap + 1) * CH, CH : 2 * CH] = zero


def toeplitz(weight):
    return local_call(toeplitz_kernel, jax.ShapeDtypeStruct((36 * CH, 2 * CH), BF16), [], 16, weight)


def spread_two(wide, base, saved, first, taps, out, at_out):
    positions = out.shape[1]
    stride = positions + 2 * ROW
    for at in range(0, positions, BLOCK):
        block = min(BLOCK, positions - at)
        lhs = jnp.concatenate(
            [
                wide[start : start + block, :]
                for frame in range(4)
                for q in range(3)
                for start in [(base + frame) * stride + at + (2 - q) * ROW]
            ],
            axis=1,
        )
        spread = jnp.dot(lhs, taps[...], preferred_element_type=F32)
        for j in range(2):
            value = saved[first + j, at : at + block, :].astype(F32)
            sigma = jax.nn.sigmoid(value)
            slope = sigma * (1.0 + value * (1.0 - sigma))
            out[at_out + j, at : at + block, :] = (spread[:, j * CH : (j + 1) * CH] * slope).astype(BF16)


def spread_mid(above, own, below, saved, taps, bands, following):
    positions = saved.shape[1]
    first = 2 if following else 0

    def kernel(above, own, below, saved, taps, *rest):
        out, wide, near, sem = rest[-4:]
        inner = near.at[:, ROW : ROW + positions, :]
        copy = pltpu.make_async_copy(saved.at[first : first + 2], inner, sem)
        copy.start()
        frames = [with_rows(above, own, below, f, f, 2) for f in range(first, 4)]
        if following:
            frames += [next_frame(rest[0], rest[1], f, 2) for f in range(2)]
        store_frames(wide, frames)
        for j in range(2):
            near[j, 0:ROW, :] = above[first + j, 2 * ROW : 3 * ROW, :]
            near[j, ROW + positions :, :] = below[first + j, 2 * ROW : 3 * ROW, :]
        copy.wait()
        spread_two(wide, 0, near, 0, taps, out, 0)

        def clear(at):
            for j in range(2):
                out[j, at : at + ROW, :] = jnp.zeros((ROW, CH), BF16)

        band = lax.axis_index(ROWS)
        pl.when(band == 0)(lambda: clear(0))
        pl.when(band == bands - 1)(lambda: clear(ROW + positions))

    extended = (2, positions + 2 * ROW, CH)
    return local_call(
        kernel,
        jax.ShapeDtypeStruct(extended, BF16),
        [
            pltpu.VMEM((4 * (positions + 4 * ROW), 3 * CH), BF16),
            pltpu.VMEM(extended, BF16),
            pltpu.SemaphoreType.DMA,
        ],
        12,
        above, own, below, saved, taps, *following,
        placed=(3,),
    )


def spread_all(low, high, later, saved, weight):
    def kernel(low, high, later, saved, weight, out, wide, taps):
        toeplitz_kernel(weight, taps)
        store_frames(wide, [whole(ref, f) for ref in (low, high, later) for f in range(2)])
        spread_two(wide, 0, saved, 0, taps, out, 0)
        spread_two(wide, 2, saved, 2, taps, out, 2)

    return local_call(
        kernel,
        jax.ShapeDtypeStruct(saved.shape, BF16),
        [pltpu.VMEM((6 * low.shape[1], 3 * CH), BF16), pltpu.VMEM((36 * CH, 2 * CH), BF16)],
        18,
        low, high, later, saved, weight,
    )


def store_share(out, total):
    planes, rows = out.shape[0], out.shape[1]
    chips, tiles = planes // 2, rows // TILE
    for plane in range(planes):
        half, chip = divmod(plane, chips)
        for start in range(0, tiles, 4):
            values = []
            for m in range(start, min(start + 4, tiles)):
                z, k = divmod(chips * m + chip, tiles)
                tap, line = divmod((2 * z + half) * rows + k * TILE, CH)
                p, tap = divmod(tap, 9)
                values.append(
                    total[p * CH + line : p * CH + line + TILE, tap * CH : (tap + 1) * CH]
                )
            size = TILE * len(values)
            out[plane, start * TILE : start * TILE + size, :] = jnp.concatenate(values).astype(BF16)


def plane_sum(pieces, depth):
    tiles = pieces.shape[1] // TILE
    chips = pieces.shape[0] // 2

    def kernel(pieces, out, total):
        value = pieces[0].astype(F32)
        for at in range(1, pieces.shape[0]):
            value += pieces[at].astype(F32)
        total[...] = value
        out[...] = jnp.zeros(out.shape, BF16)
        chip = lax.axis_index(("yl", "x"))
        for m in range(tiles):
            tile = chip + chips * m
            z, k = lax.div(tile, tiles), lax.rem(tile, tiles)
            out[z, lax.div(k, chips)] = total[m * TILE : (m + 1) * TILE, :].astype(BF16)

    out = jax.ShapeDtypeStruct((depth, SLOTS, TILE, CH), BF16)
    pieces = pltpu.with_memory_space_constraint(pieces, pltpu.HBM)
    return local_call(kernel, out, [pltpu.VMEM(pieces.shape[1:], F32)], 8, pieces)


def store_acts(turned, saved, frames):
    for at, frame in enumerate(frames):
        value = saved[frame].astype(F32)
        turned[at * CH : (at + 1) * CH, :] = (value * jax.nn.sigmoid(value)).astype(BF16).T


def add_products(total, turned, wide, frames, first_frame, first_act, acts):
    positions = turned.shape[1]
    stride = positions + 2 * ROW
    for at in range(frames):
        frame = first_frame + at
        lowest = max(0, first_act - (frame - 2))
        top = min(2, first_act + acts - 1 - (frame - 2))
        s = frame - 2 + lowest - first_act
        rhs = jnp.concatenate(
            [
                wide[start : start + positions, :]
                for q in range(3)
                for start in [at * stride + (2 - q) * ROW]
            ],
            axis=1,
        )
        lhs = turned[s * CH : (s + top - lowest + 1) * CH, :]
        total[lowest * CH : (top + 1) * CH, :] += jnp.dot(lhs, rhs, preferred_element_type=F32)


TOTAL = (3 * CH, 9 * CH)


def sum_here(above, up, below, saved):
    positions = saved.shape[1]

    def kernel(above, up, below, saved, total, wide, acts):
        store_acts(acts, saved, range(4))
        store_frames(wide, [with_rows(above, up, below, f, f, 1) for f in range(4)])
        total[...] = jnp.zeros(TOTAL, F32)
        add_products(total, acts, wide, 4, 0, 0, 4)

    return local_call(
        kernel,
        jax.ShapeDtypeStruct(TOTAL, F32),
        [
            pltpu.VMEM((4 * (positions + 2 * ROW), 3 * CH), BF16),
            pltpu.VMEM((4 * CH, positions), BF16),
        ],
        14,
        above, up, below, saved,
    )


def sums(here, edges, later, saved_second, low, high, saved_first, planes):
    positions = saved_first.shape[1]

    def kernel(here, edges, later, s2, low, high, s1, share, partial, wide, near, acts, acts_first, total):
        store_acts(acts, s2, (2, 3))
        store_frames(near, [next_frame(edges, later, f, 1) for f in range(2)])
        total[...] = here[...]
        add_products(total, acts, near, 2, 4, 2, 2)
        store_share(share, total)
        store_acts(acts_first, s1, range(4))
        store_frames(wide, [whole(ref, f) for ref in (low, high) for f in range(2)])
        partial[...] = jnp.zeros(TOTAL, F32)
        add_products(partial, acts_first, wide, 4, 0, 0, 4)

    return local_call(
        kernel,
        (
            jax.ShapeDtypeStruct((planes, 27 * CH // planes, CH), BF16),
            jax.ShapeDtypeStruct(TOTAL, F32),
        ),
        [
            pltpu.VMEM((4 * low.shape[1], 3 * CH), BF16),
            pltpu.VMEM((2 * low.shape[1], 3 * CH), BF16),
            pltpu.VMEM((2 * CH, positions), BF16),
            pltpu.VMEM((4 * CH, positions), BF16),
            pltpu.VMEM(TOTAL, F32),
        ],
        18,
        here, edges, later, saved_second, low, high, saved_first,
    )


def kept_and_sent(partial, later, saved_first, second):
    positions = saved_first.shape[1]

    def kernel(partial, later, saved, second, kept, sent, wide, acts, total):
        store_acts(acts, saved, (2, 3))
        store_frames(wide, [whole(later, f) for f in range(2)])
        total[...] = partial[...]
        add_products(total, acts, wide, 2, 4, 2, 2)

        def store(first_to, second_to):
            store_share(first_to, total)
            second_to[...] = second[...]

        core = lax.axis_index("core")
        pl.when(core == 0)(lambda: store(kept, sent))
        pl.when(core == 1)(lambda: store(sent, kept))

    out = jax.ShapeDtypeStruct(second.shape, BF16)
    return local_call(
        kernel,
        (out, out),
        [
            pltpu.VMEM((2 * later.shape[1], 3 * CH), BF16),
            pltpu.VMEM((2 * CH, positions), BF16),
            pltpu.VMEM(TOTAL, F32),
        ],
        12,
        partial, later, saved_first, second,
    )


def moved(block, axis, step):
    count = lax.axis_size(axis)
    route = [(i, i + step) for i in range(count) if 0 <= i + step < count]
    return lax.ppermute(block, axis, route)


def exchanged(pieces, axis):
    return lax.all_to_all(pieces, axis, split_axis=0, concat_axis=0, tiled=True)


def body(upstream, saved_first, saved_second, weight_first, weight_second):
    frames, height, width, chans = upstream.shape
    planes, depth = lax.axis_size(PLANE), lax.axis_size("z")
    flat = lambda a: a.reshape(frames, height * width, chans)
    up, s1, s2 = flat(upstream), flat(saved_first), flat(saved_second)

    bands = lax.axis_size(ROWS)

    size = up.shape[1]
    tail, head, start, up_near, s2_near = copied(
        (
            (0, rows_of(4, 0, 2 * ROW), 0, rows_of(4, size - 2 * ROW, 2 * ROW)),
            (0, rows_of(4, 2 * ROW, ROW), 1, rows_of(4, size - ROW, ROW)),
            (1, rows_of(4, 0, 2 * ROW), 0, rows_of(4, 0, 2 * ROW)),
            (1, rows_of(4, 2 * ROW, ROW), 1, rows_of(4, 0, ROW)),
            (2, rows_of(2, 0, size), 0, rows_of(2, 0, size)),
            (3, rows_of(4, 0, size), 0, rows_of(4, 0, size)),
            (4, rows_of(4, 0, size), 1, rows_of(4, 0, size)),
        ),
        ((frames, 3 * ROW, CH), (frames, 3 * ROW, CH), (2, size, CH), up.shape, up.shape),
        tuple(pltpu.with_memory_space_constraint(a, pltpu.HBM) for a in (up, s2)),
        pltpu.HBM,
    )
    above = moved(tail, ROWS, 1)
    below = moved(head, ROWS, -1)
    later = moved(start, TM, -1)
    (packed,) = copied(
        (
            (0, rows_of(2, 0, 2 * ROW), 0, rows_of(2, 0, 2 * ROW)),
            (0, rows_of(2, 2 * ROW, 2 * ROW), 1, rows_of(2, 0, 2 * ROW)),
        ),
        ((2, 4 * ROW, CH),),
        (above, below),
        pl.ANY,
    )
    edges = moved(packed, TM, -1)
    taps_second = toeplitz(weight_second)
    low = spread_mid(above, up_near, below, s2_near, taps_second, bands, ())
    mid_later = moved(low, TM, -1)
    here = sum_here(above, up_near, below, s2_near)
    high = spread_mid(
        above, up_near, below, s2_near, taps_second, bands, (edges, later)
    )
    second, partial = sums(here, edges, later, s2_near, low, high, s1, planes)
    kept, sent = kept_and_sent(partial, mid_later, s1, second)
    received = lax.ppermute(sent, "core", [(0, 1), (1, 0)])
    half = added(kept, received)
    part = exchanged(half, PLANE)
    part = plane_sum(part, depth)
    grad_input = spread_all(low, high, mid_later, s1, weight_first)
    part = exchanged(part, "z")
    factor = 1.0 / math.sqrt(frames * lax.axis_size(TM) * height * bands * width)
    every = exchanged(summed_copies(part, bands, factor), ROWS)
    share_first, share_second = shares(every, weight_first.shape[0] // lax.axis_size(TM))
    return (grad_input.reshape(upstream.shape), share_first, share_second)


def solution(mesh):
    finer = Mesh(mesh.devices.reshape(8, 2, 2, 4, 2), ("z", "yh", "yl", "x", "core"))
    field = P(TM, ROWS, None, None)
    in_specs = (field, field, field, P(), P())
    out_specs = (field, P(TM, None), P(TM, None))
    return jax.shard_map(body, mesh=finer, in_specs=in_specs, out_specs=out_specs, check_vma=False)
```
